256 devices in a mesh: dp: 128 (over z, x_hi, y, core), mp: 2 (over x_lo).
Axes of the slice: x: 4 (x_hi: 2, x_lo: 2; x = x_hi * 2 + x_lo), y: 4, z: 8, core: 2. Of those that a mesh axis runs over, the one named last changes fastest.
Arguments:
- image_feat: bfloat16 [16384, 1024], P('dp', 'mp'), may hold values from -6 to 6
- image_proj: bfloat16 [1024, 768], P('mp'), may hold values from -1 to 1
- text_feat: bfloat16 [16384, 768], P('dp', 'mp'), may hold values from -6 to 6
- text_proj: bfloat16 [768, 768], P('mp'), may hold values from -1 to 1
- pair_index: int32 [16384], P('dp'), may hold values from 0 to 16383, each once
- logit_scale: float32 [1], replicated, may hold values from 10 to 100
Outputs:
- row_loss: float32 [16384], P('dp')
- col_loss: float32 [16384], P(('dp', 'mp'))
The draws below stay inside these ranges and needn't reach their ends.
Inputs may be any that keep to these rules, and one draw needn't show every extreme that they name: `pair_index`: each text index appears exactly once.
All inputs are finite; a program needn't handle non-finite values.
Results may differ from the reference program's by a relative error of at most 0.00091.
Values may be sent and summed in bfloat16 or wider, within the bound.
A program may use at most 64 MiB of HBM per device.

```python
import jax
import jax.numpy as jnp
from jax import lax

WIDTH = 1024
TEXT_WIDTH = 768
EMB = 768
TOKENS = 16384


feature_bound = 6.0


weight_bound = 1.0


def image_weights(key):
    values = jax.random.normal(jax.random.fold_in(key, 11), (WIDTH, EMB), jnp.float32) * WIDTH ** (-0.5)
    return jnp.clip(values, -weight_bound, weight_bound)


def text_weights(key):
    values = jax.random.normal(jax.random.fold_in(key, 12), (TEXT_WIDTH, EMB), jnp.float32) * TEXT_WIDTH ** (-0.5)
    return jnp.clip(values, -weight_bound, weight_bound)


def text_inputs(key):
    features = jnp.clip(jax.random.normal(jax.random.fold_in(key, 13), (TOKENS, TEXT_WIDTH), jnp.float32), -feature_bound, feature_bound)
    return features


def draw_image_proj(key, part):
    return image_weights(key).astype(jnp.bfloat16)


def draw_text_proj(key, part):
    return text_weights(key).astype(jnp.bfloat16)


def draw_text_feat(key, part):
    return text_inputs(key).astype(jnp.bfloat16)


def draw_image_feat(key, part):
    features = jnp.clip(jax.random.normal(jax.random.fold_in(key, 16), (TOKENS, WIDTH), jnp.float32), -feature_bound, feature_bound)
    return features.astype(jnp.bfloat16)


def draw_logit_scale(key, part):
    value = jnp.exp(jax.random.uniform(jax.random.fold_in(key, 17), (1,), jnp.float32, jnp.log(10.0), jnp.log(100.0)))
    return jnp.clip(value, 10.0, 100.0)


def setup_inputs(seed: int = 0) -> dict:
    splits = jax.random.split(jax.random.key(seed), 7)
    return {
        "image_feat": draw_image_feat(jax.random.fold_in(splits[6], 71), 0),
        "image_proj": draw_image_proj(jax.random.fold_in(splits[6], 71), 0),
        "text_feat": draw_text_feat(jax.random.fold_in(splits[6], 71), 0),
        "text_proj": draw_text_proj(jax.random.fold_in(splits[6], 71), 0),
        "pair_index": jax.random.permutation(splits[4], TOKENS).astype(jnp.int32),
        "logit_scale": draw_logit_scale(jax.random.fold_in(splits[6], 71), 0),
    }


def embed(features, projection):
    raw = jnp.dot(features.astype(jnp.float32), projection.astype(jnp.float32), preferred_element_type=jnp.float32)
    norm_sq = lax.optimization_barrier(jnp.sum(raw * raw, axis=1, keepdims=True))
    return (raw / jnp.sqrt(norm_sq + 1e-06)).astype(jnp.bfloat16)

def reference(image_feat, image_proj, text_feat, text_proj, pair_index, logit_scale):
    image_emb = embed(image_feat, image_proj)
    text_emb = embed(text_feat, text_proj)
    multiplier = logit_scale[0]
    block_rows = min(1024, TOKENS)
    block_count = TOKENS // block_rows

    def row_block(index):
        rows = lax.dynamic_slice_in_dim(image_emb, index * block_rows, block_rows, 0)
        logits = multiplier * lax.dot_general(rows.astype(jnp.float32), text_emb.astype(jnp.float32), (((1,), (1,)), ((), ())), preferred_element_type=jnp.float32)
        return jax.nn.logsumexp(logits, axis=1)

    def col_block(index):
        cols = lax.dynamic_slice_in_dim(text_emb, index * block_rows, block_rows, 0)
        logits = multiplier * lax.dot_general(cols.astype(jnp.float32), image_emb.astype(jnp.float32), (((1,), (1,)), ((), ())), preferred_element_type=jnp.float32)
        return jax.nn.logsumexp(logits, axis=1)
    indices = jnp.arange(block_count, dtype=jnp.int32)
    row_lse = lax.map(row_block, indices).reshape(TOKENS)
    col_lse = lax.map(col_block, indices).reshape(TOKENS)
    paired = text_emb[pair_index].astype(jnp.float32)
    positive = multiplier * lax.optimization_barrier(jnp.sum(image_emb.astype(jnp.float32) * paired, axis=1))
    col_positive = jnp.zeros((TOKENS,), jnp.float32).at[pair_index].set(positive)
    return (row_lse - positive, col_lse - col_positive)
```

```python
import functools
import math

import jax
import jax.numpy as jnp
from jax import lax
from jax.experimental import pallas as pl
from jax.experimental.pallas import tpu as pltpu
from jax.sharding import PartitionSpec as P

MESH = pl.DeviceIdType.MESH
F32 = jnp.float32
BF16 = jnp.bfloat16

NX, NY, NZ, NC = 4, 4, 8, 2
ROWS = 64
EMB = 768
TILE = 1024
HIGH, LOW, CLAMP = 34.0, 20.0, 90.0
LN2 = math.log(2.0)


def device(x, y, z, c):
    dp = ((z * 2 + lax.div(x, 2)) * NY + y) * NC + c
    return (dp, lax.rem(x, 2))


def kernel(
    fi_hbm, pi_hbm, ft_hbm, pt_hbm, pair_hbm, scale_ref,
    row_ref, col_ref,
    fi, pi, ft, pt, part_i, part_t, send_i, send_t, got_i, got_t,
    img, txt, pair, logit, colsum, rowstat, colstat, rows_in, cols_in,
    load_sem, exch_send, exch_recv, img_send, img_recv, txt_send, txt_recv,
    pair_send, pair_recv, rs_send, rs_recv, cs_send, cs_recv,
):
    dp, mp = lax.axis_index("dp"), lax.axis_index("mp")
    c = lax.rem(dp, 2)
    y = lax.rem(lax.div(dp, 2), NY)
    xh = lax.rem(lax.div(dp, 8), 2)
    z = lax.div(dp, 16)
    x = xh * 2 + mp
    shard = xh * NY + y
    slot = shard * 2 + mp
    cslot = c * NZ + z

    def slot_of(xx, yy):
        return (lax.div(xx, 2) * NY + yy) * 2 + lax.rem(xx, 2)

    loads = []
    for k, (src, dst) in enumerate(((fi_hbm, fi), (pi_hbm, pi), (ft_hbm, ft), (pt_hbm, pt), (pair_hbm, pair.at[shard]))):
        copy = pltpu.make_async_copy(src, dst, load_sem.at[k])
        copy.start()
        loads.append(copy)

    plane = []
    for dx in range(NX):
        for dy in range(NY):
            if dx or dy:
                plane.append((lax.rem(x + dx, NX), lax.rem(y + dy, NY)))
    column = []
    for dz in range(NZ):
        for dc in range(NC):
            if dz or dc:
                column.append((lax.rem(z + dz, NZ), lax.rem(c + dc, NC)))

    barrier = pltpu.get_barrier_semaphore()
    for px, py in plane:
        pl.semaphore_signal(barrier, inc=1, device_id=device(px, py, z, c), device_id_type=MESH)
    for pz, pc in column:
        pl.semaphore_signal(barrier, inc=1, device_id=device(x, y, pz, pc), device_id_type=MESH)

    started = []

    def send(src, dst, send_sem, recv_sem, to):
        copy = pltpu.make_async_remote_copy(
            src_ref=src, dst_ref=dst, send_sem=send_sem, recv_sem=recv_sem, device_id=to, device_id_type=MESH
        )
        copy.start()
        started.append(copy)

    sibling = device(x, y, z, 1 - c)

    def arrived(dst, recv_sem):
        pltpu.make_async_remote_copy(
            src_ref=dst, dst_ref=dst, send_sem=exch_send.at[0], recv_sem=recv_sem, device_id=sibling, device_id_type=MESH
        ).wait_recv()

    own = pl.ds(pl.multiple_of(mp * ROWS, ROWS), ROWS)
    other = pl.ds(pl.multiple_of((1 - mp) * ROWS, ROWS), ROWS)
    partner = device(xh * 2 + 1 - mp, y, z, c)

    loads[0].wait()
    loads[1].wait()
    part_i[...] = jnp.dot(fi[...], pi[...], preferred_element_type=F32)
    send_i[...] = part_i[other, :].astype(BF16)
    pl.semaphore_wait(barrier, len(plane) + len(column))
    send(send_i, got_i, exch_send.at[0], exch_recv.at[0], partner)
    loads[2].wait()
    loads[3].wait()
    part_t[...] = jnp.dot(ft[...], pt[...], preferred_element_type=F32)
    send_t[...] = part_t[other, :].astype(BF16)
    send(send_t, got_t, exch_send.at[1], exch_recv.at[1], partner)
    loads[4].wait()
    n_pair = 0
    for px, py in plane:
        pass
    for dxh in range(2):
        for dy in range(NY):
            if dxh or dy:
                to = device(lax.rem(xh + dxh, 2) * 2 + mp, lax.rem(y + dy, NY), z, c)
                send(pair.at[shard], pair.at[shard], pair_send.at[n_pair], pair_recv.at[shard], to)
                n_pair += 1

    def normalize(raw):
        norm_sq = jnp.sum(raw * raw, axis=1, keepdims=True)
        return (raw / jnp.sqrt(norm_sq + 1e-06)).astype(BF16)

    def img_at(s, half):
        return img.at[pl.ds(pl.multiple_of(s * ROWS + half * 32, 32), 32), :]

    def txt_at(cs, zs, half):
        return txt.at[pl.ds(pl.multiple_of((cs * NZ + zs) * ROWS + half * 32, 32), 32), :]

    count = {"img": 0, "txt": 0}

    def send_img(s, half, to):
        send(img_at(s, half), img_at(s, half), img_send.at[count["img"]], img_recv.at[s * 2 + half], to)
        count["img"] += 1

    def send_txt(cs, zs, half, to):
        send(
            txt_at(cs, zs, half), txt_at(cs, zs, half), txt_send.at[count["txt"]],
            txt_recv.at[(cs * NZ + zs) * 2 + half], to,
        )
        count["txt"] += 1

    along_x = [device(lax.rem(x + d, NX), y, z, c) for d in (1, 3, 2)]
    along_y = [device(x, lax.rem(y + d, NY), z, c) for d in (1, 3, 2)]
    up, down = device(x, y, lax.rem(z + 1, NZ), c), device(x, y, lax.rem(z + NZ - 1, NZ), c)

    arrived(got_i, exch_recv.at[0])
    img[pl.ds(pl.multiple_of(slot * ROWS, ROWS), ROWS), :] = normalize(part_i[own, :] + got_i[...].astype(F32))
    for kx, ky in zip(along_x, along_y):
        send_img(slot, 0, kx)
        send_img(slot, 1, ky)
    for kx, ky in zip(along_x, along_y):
        send_img(slot, 0, ky)
        send_img(slot, 1, kx)

    arrived(got_t, exch_recv.at[1])
    txt[pl.ds(pl.multiple_of(cslot * ROWS, ROWS), ROWS), :] = normalize(part_t[own, :] + got_t[...].astype(F32))
    for half in range(2):
        send_txt(c, z, half, up)
        send_txt(c, z, half, down)
    for half in range(2):
        send_txt(c, z, half, sibling)

    def relay_img(d):
        sx = slot_of(lax.rem(x + d, NX), y)
        arrived(img_at(sx, 0), img_recv.at[sx * 2])
        for ky in along_y:
            send_img(sx, 0, ky)
        sy = slot_of(x, lax.rem(y + d, NY))
        arrived(img_at(sy, 1), img_recv.at[sy * 2 + 1])
        for kx in along_x:
            send_img(sy, 1, kx)

    def relay_txt(k, half):
        below, above = lax.rem(z + NZ - k, NZ), lax.rem(z + k, NZ)
        if k < 4 or half == 0:
            arrived(txt_at(c, below, half), txt_recv.at[(c * NZ + below) * 2 + half])
            if k < 3 or (k == 3 and half == 0):
                send_txt(c, below, half, up)
            send_txt(c, below, half, sibling)
        if k < 4 or half == 1:
            arrived(txt_at(c, above, half), txt_recv.at[(c * NZ + above) * 2 + half])
            if k < 3 or (k == 3 and half == 1):
                send_txt(c, above, half, down)
            send_txt(c, above, half, sibling)

    relay_img(1)
    relay_img(3)
    relay_txt(1, 0)
    relay_txt(1, 1)
    relay_img(2)
    for k in (2, 3, 4):
        relay_txt(k, 0)
        relay_txt(k, 1)

    for dx in range(1, NX):
        for dy in range(1, NY):
            s = slot_of(lax.rem(x + dx, NX), lax.rem(y + dy, NY))
            for half in range(2):
                arrived(img_at(s, half), img_recv.at[s * 2 + half])
    for d in range(1, NX):
        sx = slot_of(lax.rem(x + d, NX), y)
        arrived(img_at(sx, 1), img_recv.at[sx * 2 + 1])
        sy = slot_of(x, lax.rem(y + d, NY))
        arrived(img_at(sy, 0), img_recv.at[sy * 2])
    for zs in range(NZ):
        for half in range(2):
            arrived(txt_at(1 - c, zs, half), txt_recv.at[((1 - c) * NZ + zs) * 2 + half])
    for dxh in range(2):
        for dy in range(NY):
            if dxh or dy:
                q = lax.rem(xh + dxh, 2) * NY + lax.rem(y + dy, NY)
                arrived(pair.at[q], pair_recv.at[q])

    scale = scale_ref[0]
    to_log2 = scale * (1.0 / LN2)
    sub = lax.broadcasted_iota(jnp.int32, (32, 128), 0)
    zero = jnp.zeros((8, 128), F32)
    row_a, row_b, row_p = [zero] * 8, [zero] * 8, [zero] * 8
    step = 256
    for m in range(TILE // step):
        buf = m % 2
        logit[buf] = lax.dot_general(
            txt[m * step : (m + 1) * step, :], img[...], (((1,), (1,)), ((), ())), preferred_element_type=F32
        )
        for g in range(step // 32):
            at = m * step + g * 32
            cs, zs, r = at // 512, at // 64 % 8, at % 64
            text = sub + (zs * 2048 + cs * 128 + r) + (xh * 1024 + y * 256 + mp * 64)
            col_a = col_b = col_p = jnp.zeros((32, 128), F32)
            for q in range(8):
                acc = logit[buf, g * 32 : (g + 1) * 32, q * 128 : (q + 1) * 128]
                power = acc * to_log2
                a = jnp.exp2(power - HIGH)
                b = jnp.exp2(jnp.minimum(power, CLAMP) + LOW)
                p = jnp.where(pair[q] == text, acc, 0.0)
                col_a, col_b, col_p = col_a + a, col_b + b, col_p + p
                row_a[q] = row_a[q] + a.reshape(4, 8, 128).sum(axis=0)
                row_b[q] = row_b[q] + b.reshape(4, 8, 128).sum(axis=0)
                row_p[q] = row_p[q] + p.reshape(4, 8, 128).sum(axis=0)
            colsum[0, at : at + 32, :] = col_a
            colsum[1, at : at + 32, :] = col_b
            colsum[2, at : at + 32, :] = col_p

    line = lax.broadcasted_iota(jnp.int32, (8, 128), 0)

    def three(a, b, p):
        return jnp.where(line == 0, a, jnp.where(line == 1, b, jnp.where(line == 2, p, 0.0)))

    for q in range(8):
        sums = [jnp.sum(v[q], axis=0, keepdims=True) for v in (row_a, row_b, row_p)]
        rowstat[q] = three(*sums)
    for n, (px, py) in enumerate(plane):
        q = lax.div(px, 2) * NY + py
        send(rowstat.at[q], rows_in.at[slot], rs_send.at[n], rs_recv.at[slot], device(px, py, z, c))
    for blk in range(8):
        sums = [
            jnp.sum(colsum[k, blk * 128 : (blk + 1) * 128, :].T, axis=0, keepdims=True) for k in range(3)
        ]
        colstat[blk] = three(*sums)
    for n, (pz, pc) in enumerate(column):
        blk = pc * 4 + lax.div(pz, 2)
        send(colstat.at[blk], cols_in.at[cslot], cs_send.at[n], cs_recv.at[cslot], device(x, y, pz, pc))

    def loss(total):
        high, low, positive = total[0:1], total[1:2], total[2:3]
        lse = jnp.where(high > 2.0**-HIGH, jnp.log(high) + HIGH * LN2, jnp.log(low) - LOW * LN2)
        return lse - scale * positive

    total = rowstat[shard]
    for px, py in plane:
        s = slot_of(px, py)
        arrived(rows_in.at[s], rs_recv.at[s])
        total = total + rows_in[s]
    row_ref[...] = loss(total)
    total = colstat[c * 4 + lax.div(z, 2)]
    for pz, pc in column:
        s = pc * NZ + pz
        arrived(cols_in.at[s], cs_recv.at[s])
        total = total + cols_in[s]
    both = loss(total)
    col_ref[...] = jnp.where(lax.rem(z, 2) == 0, both[:, :ROWS], both[:, ROWS:])

    for copy in started:
        copy.wait_send()


def on_device(image_feat, image_proj, text_feat, text_proj, pair_index, logit_scale):
    dma = pltpu.SemaphoreType.DMA
    anywhere = pl.BlockSpec(memory_space=pl.ANY)
    vmem = pl.BlockSpec(memory_space=pltpu.VMEM)
    row, col = pl.pallas_call(
        kernel,
        out_shape=(jax.ShapeDtypeStruct((1, 2 * ROWS), F32), jax.ShapeDtypeStruct((1, ROWS), F32)),
        in_specs=[anywhere] * 5 + [pl.BlockSpec(memory_space=pltpu.SMEM)],
        out_specs=(vmem, vmem),
        scratch_shapes=[
            pltpu.VMEM(image_feat.shape, BF16),
            pltpu.VMEM(image_proj.shape, BF16),
            pltpu.VMEM(text_feat.shape, BF16),
            pltpu.VMEM(text_proj.shape, BF16),
            pltpu.VMEM((2 * ROWS, EMB), F32),
            pltpu.VMEM((2 * ROWS, EMB), F32),
            pltpu.VMEM((ROWS, EMB), BF16),
            pltpu.VMEM((ROWS, EMB), BF16),
            pltpu.VMEM((ROWS, EMB), BF16),
            pltpu.VMEM((ROWS, EMB), BF16),
            pltpu.VMEM((TILE, EMB), BF16),
            pltpu.VMEM((TILE, EMB), BF16),
            pltpu.VMEM((8, 1, 128), jnp.int32),
            pltpu.VMEM((2, 256, TILE), F32),
            pltpu.VMEM((3, TILE, 128), F32),
            pltpu.VMEM((8, 8, 128), F32),
            pltpu.VMEM((8, 8, 128), F32),
            pltpu.VMEM((16, 8, 128), F32),
            pltpu.VMEM((16, 8, 128), F32),
            dma((5,)), dma((2,)), dma((2,)), dma((30,)), dma((32,)), dma((30,)), dma((32,)),
            dma((7,)), dma((8,)), dma((15,)), dma((16,)), dma((15,)), dma((16,)),
        ],
        compiler_params=pltpu.CompilerParams(
            collective_id=0, has_side_effects=True, vmem_limit_bytes=60 * 1024 * 1024
        ),
        name="contrastive",
    )(image_feat, image_proj, text_feat, text_proj, pair_index.reshape(1, 2 * ROWS), logit_scale)
    return row.reshape(2 * ROWS), col.reshape(ROWS)


def solution(mesh):
    in_specs = (P("dp", "mp"), P("mp", None), P("dp", "mp"), P("mp", None), P("dp"), P())
    out_specs = (P("dp"), P(("dp", "mp")))
    return jax.shard_map(on_device, mesh=mesh, in_specs=in_specs, out_specs=out_specs, check_vma=False)
```
